128 devices in a mesh: wide: 16 (over x_hi, y, core), narrow: 8 (over z, x_lo).
Axes of the slice: x: 4 (x_hi: 2, x_lo: 2; x = x_hi * 2 + x_lo), y: 4, z: 4, core: 2. Of those that a mesh axis runs over, the one named last changes fastest.
Arguments:
- image: bfloat16 [2, 256, 256, 256], P(None, 'wide', 'narrow'), may hold values from -6 to 6
- deapodization: float32 [3, 256], replicated, may hold values from 0.5 to 2
- offsets: int32 [128, 16], P(('wide', 'narrow')), may hold values from 0 to 256
- cross_weight: bfloat16 [128, 16, 1536, 256], P(('wide', 'narrow')), may hold values from -0.375 to 0.375
- x_weight: bfloat16 [128, 16, 1536, 256], P(('wide', 'narrow')), may hold values from -0.375 to 0.375
Outputs:
- samples: float32 [128, 16, 2, 1536], P(('wide', 'narrow'))
The draws below stay inside these ranges and needn't reach their ends.
Inputs may be any that keep to these rules, and one draw needn't show every extreme that they name: `offsets`: each entry is the first row, along the first frequency dimension, of a group's window of 256 rows in one slab.
All inputs are finite; a program needn't handle non-finite values.
Results may differ from the reference program's by a relative error of at most 0.007.
Values may be sent and summed in bfloat16 or wider, within the bound.
No kernel may reach another device: no remote copies, remote signals or barrier semaphores. Data moves between devices by JAX's collectives and lax.ppermute only.
A program may use at most 128 MiB of HBM per device.

```python
import math
import jax
import jax.numpy as jnp
from jax import lax

N = 256
G = 512
KZ = 64
BX = 256
SAMP = 1536
CROSS = 256
GROUPS = 128
N_WIDE = 16
N_NARROW = 8


def plant(array, stream_key, least, high):
    place = [jax.random.randint(jax.random.fold_in(stream_key, axis), (), 0, length) for axis, length in enumerate(array.shape)]
    longest = array.shape.index(max(array.shape))
    beside = place[:longest] + [(place[longest] + 1) % array.shape[longest]] + place[longest + 1:]
    return array.at[tuple(place)].set(least).at[tuple(beside)].set(high)


def steps_of(key, shape, cuts, least, high):
    level = 1.0
    for axis_at, shards_of in cuts:
        heights = jax.random.uniform(jax.random.fold_in(jax.random.fold_in(key, 6), axis_at), (shards_of,), jnp.float32, least / len(cuts), high / len(cuts))
        level = level * jnp.repeat(jnp.exp(heights), shape[axis_at] // shards_of).reshape((-1,) + (1,) * (len(shape) - 1 - axis_at))
    return level


def normal_values(key, dims, width, most, split=(), held_as=jnp.bfloat16):
    result = jax.random.normal(key, dims, jnp.float32) * width
    if len(split) > 0:
        result = steps_of(key, dims, split, -0.22, 0.18) * result
    return jnp.clip(result, min=-most, max=most).astype(held_as)


def setup_inputs(seed: int = 0) -> dict:
    arg_keys = jax.random.split(jax.random.key(seed), 6)
    return {
        "image": normal_values(arg_keys[0], (2, N, N, N), 1.0, 6.0, ((1, 16), (2, 8))),
        "deapodization": jnp.clip(jnp.exp(jax.random.uniform(arg_keys[1], (3, N), jnp.float32, math.log(0.5), math.log(2.0))), 0.5, 2.0),
        "offsets": plant(jax.random.randint(arg_keys[2], (GROUPS, N_WIDE), 0, G - BX + 1), jax.random.fold_in(arg_keys[2], 1), 0, G - BX).astype(jnp.int32),
        "cross_weight": normal_values(arg_keys[3], (GROUPS, N_WIDE, SAMP, CROSS), CROSS ** -0.5, 0.375, ((0, 128),)),
        "x_weight": normal_values(arg_keys[4], (GROUPS, N_WIDE, SAMP, BX), BX ** -0.5, 0.375, ((0, 128),)),
    }


def dft_tables(out_rows, inputs, grid_size, lowest):
    frequency = jnp.arange(out_rows, dtype=jnp.int32) + lowest
    position = jnp.arange(inputs, dtype=jnp.int32) - inputs // 2
    phases = jnp.mod(frequency[:, None] * position[None, :], grid_size)
    angles = phases.astype(jnp.float32) * (2.0 * math.pi / grid_size)
    factor = 1.0 / math.sqrt(inputs)
    return jnp.stack([jnp.cos(angles) * factor, jnp.sin(angles) * factor]).astype(jnp.bfloat16)

def mix_parts(product):
    return (product[0, 0] + product[1, 1], product[0, 1] - product[1, 0])

def reference(image, deapodization, offsets, cross_weight, x_weight):
    weighted = (image.astype(jnp.float32) * deapodization[0][None, :, None, None] * deapodization[1][None, None, :, None] * deapodization[2][None, None, None, :]).astype(jnp.bfloat16)
    z_table = dft_tables(KZ, N, G, -(KZ // 2)).astype(jnp.float32)
    product = jnp.einsum('tkz,cxyz->tcxyk', z_table, weighted.astype(jnp.float32))
    real_part, imag_part = mix_parts(product)
    band_data = jnp.stack([real_part, imag_part], axis=0).astype(jnp.bfloat16)
    line_table = dft_tables(G, N, G, -(G // 2)).astype(jnp.float32)
    product = jnp.einsum('tqy,cxyk->tcxqk', line_table, band_data.astype(jnp.float32))
    real_part, imag_part = mix_parts(product)
    columns = jnp.stack([real_part, imag_part], axis=0).astype(jnp.bfloat16)
    product = jnp.einsum('tpx,cxqk->tcpqk', line_table, columns.astype(jnp.float32))
    real_part, imag_part = mix_parts(product)
    kspace = jnp.stack([real_part, imag_part], axis=1).astype(jnp.bfloat16)
    span_y = G // N_WIDE
    span_z = KZ // N_NARROW

    def group_samples(group_index):
        narrow_pos = group_index % N_NARROW

        def slab_samples(slab_index):
            start_row = offsets[group_index, slab_index]
            window_rows = lax.dynamic_slice(kspace, (start_row, jnp.int32(0), slab_index * span_y, narrow_pos * span_z), (BX, 2, span_y, span_z)).reshape(BX, 2, span_y * span_z)
            cross_rows = cross_weight[group_index, slab_index].astype(jnp.float32)
            partial_value = jnp.einsum('ms,qcs->cmq', cross_rows, window_rows.astype(jnp.float32))
            window_gain = x_weight[group_index, slab_index].astype(jnp.float32)
            return lax.optimization_barrier(jnp.sum(partial_value * window_gain[None], axis=-1))
        return lax.map(slab_samples, jnp.arange(N_WIDE, dtype=jnp.int32))
    return lax.map(group_samples, jnp.arange(N_WIDE * N_NARROW, dtype=jnp.int32))
```

```python
import math

import jax
import jax.numpy as jnp
import numpy as np
from jax import lax
from jax.experimental import pallas as pl
from jax.experimental.pallas import tpu as pltpu
from jax.sharding import PartitionSpec as P

N = 256
G = 512
KZ = 64
SAMP = 1536
SLABS = 16
NARROW = 8
CHIPS = 8
XB = 16
YB = 32
ZB = KZ // NARROW


def trig(frequency, position):
    phase = np.mod(np.asarray(frequency, np.int64)[:, None] * np.asarray(position, np.int64)[None, :], G)
    angle = phase.astype(np.float32) * np.float32(2.0 * math.pi / G)
    factor = np.float32(1.0 / math.sqrt(N))
    return (np.cos(angle) * factor).astype(np.float32), (np.sin(angle) * factor).astype(np.float32)


def complex_table(cosine, sine):
    real = np.stack([cosine, sine], axis=1)
    imag = np.stack([-sine, cosine], axis=1)
    return np.stack([real, imag], axis=0)


def tables():
    position = np.arange(N) - N // 2
    z = complex_table(*trig(np.arange(KZ) - KZ // 2, position))
    z = z.reshape(2, NARROW, ZB, 2, N).transpose(3, 4, 2, 1, 0).reshape(2 * N, ZB * NARROW * 2)
    y = complex_table(*trig(np.arange(G) - G // 2, position))
    y = y.reshape(2, G, 2, NARROW, YB).transpose(0, 1, 3, 2, 4).reshape(2 * G, 2 * N)
    x = complex_table(*trig(np.arange(N) - G // 2, position)).reshape(2 * N, 2 * N)
    offset = np.arange(N + 8)
    pc, ps = trig(offset, position)
    phase = np.concatenate([pc, ps], axis=1) * np.float32(math.sqrt(N))
    as_bf16 = lambda t: jnp.asarray(t, jnp.float32).astype(jnp.bfloat16)
    return as_bf16(z), as_bf16(y), as_bf16(x), jnp.asarray(phase, jnp.float32)


def nt(a, b):
    return lax.dot_general(a, b, (((1,), (1,)), ((), ())), preferred_element_type=jnp.float32)


def band_kernel(scale_s, scale_v, image, z_table, out, rows):
    wide = lax.axis_index("wide")
    narrow = lax.axis_index("narrow")
    lane = lax.broadcasted_iota(jnp.int32, (YB, N), 1)
    row = lax.broadcasted_iota(jnp.int32, (YB, N), 0)
    picked = jnp.where(lane == row + narrow * YB, scale_v[1:2, :], 0.0)
    scale_y = jnp.sum(picked, axis=1, keepdims=True)
    scale_z = scale_v[2:3, :]
    for x in range(XB):
        scale_x = scale_s[0, wide * XB + x]
        for c in range(2):
            value = image[c, x].astype(jnp.float32) * scale_x * scale_y * scale_z
            rows[x * YB:(x + 1) * YB, c * N:(c + 1) * N] = value.astype(jnp.bfloat16)
    product = jnp.dot(rows[...], z_table[...], preferred_element_type=jnp.float32)
    part = [product[x * YB:(x + 1) * YB] for x in range(XB)]
    lanes = lax.broadcasted_iota(jnp.int32, (YB, 128), 1)
    for bit in range(4):
        d = 1 << bit
        low = (lanes & d) == 0
        for i in range(XB):
            if i & d:
                continue
            a, b = part[i], part[i | d]
            part[i] = jnp.where(low, a, pltpu.roll(b, d, 1))
            part[i | d] = jnp.where(low, pltpu.roll(a, 128 - d, 1), b)
    for g in range(2 * NARROW):
        value = part[g].astype(jnp.bfloat16)
        for chip in range(CHIPS):
            out[chip, g // 2, (g % 2) * YB:(g % 2 + 1) * YB, :] = value


def sample_kernel(offsets, mine, other, y_table, x_table, phase, cross_hbm, gain_hbm, out,
                  band, columns, cross, gain, cross_sem, gain_sem):
    for s in range(SLABS):
        pltpu.make_async_copy(cross_hbm.at[s], cross.at[s], cross_sem.at[s]).start()
        pltpu.make_async_copy(gain_hbm.at[s], gain.at[s], gain_sem.at[s]).start()
    core = lax.rem(lax.axis_index("wide"), 2)
    for side, source in ((core, mine), (1 - core, other)):
        for chip in range(CHIPS):
            turned = source[chip].T
            start = pl.multiple_of((2 * chip + side) * XB, XB)
            for k in range(ZB):
                band[k, pl.ds(start, XB), :] = turned[k * XB:(k + 1) * XB]
    for k in range(ZB):
        lines = nt(y_table[...], band[k])
        for part in range(4):
            piece = lines[part // 2 * G:(part // 2 + 1) * G, part % 2 * 128:(part % 2 + 1) * 128]
            columns[part, pl.ds(k, G, stride=ZB), :] = piece

    def slab(s, carry):
        turn = phase[pl.ds(offsets[0, s], 1), :]
        start = pl.multiple_of(s * N, N)
        turned = []
        for half in range(2):
            cosine = turn[:, half * 128:(half + 1) * 128]
            sine = turn[:, N + half * 128:N + (half + 1) * 128]
            real = columns[half, pl.ds(start, N), :]
            imag = columns[2 + half, pl.ds(start, N), :]
            turned.append((real * cosine + imag * sine).astype(jnp.bfloat16))
            turned.append((imag * cosine - real * sine).astype(jnp.bfloat16))
        turned = jnp.concatenate([turned[0], turned[2], turned[1], turned[3]], axis=1)
        window = nt(x_table[...], turned).astype(jnp.bfloat16)
        pltpu.make_async_copy(cross_hbm.at[s], cross.at[s], cross_sem.at[s]).wait()
        pltpu.make_async_copy(gain_hbm.at[s], gain.at[s], gain_sem.at[s]).wait()
        for t in range(SAMP // N):
            cut = slice(t * N, (t + 1) * N)
            partial = nt(window, cross[s, cut, :])
            weight = gain[s, cut, :].T.astype(jnp.float32)
            out[s, 0:1, cut] = jnp.sum(partial[:N] * weight, axis=0, keepdims=True)
            out[s, 1:2, cut] = jnp.sum(partial[N:] * weight, axis=0, keepdims=True)
        return carry

    lax.fori_loop(0, SLABS, slab, 0)


def per_device(image, deapodization, offsets, cross_weight, x_weight):
    z_table, y_table, x_table, phase = tables()
    vmem = pl.BlockSpec(memory_space=pltpu.VMEM)
    smem = pl.BlockSpec(memory_space=pltpu.SMEM)
    hbm = pl.BlockSpec(memory_space=pl.ANY)
    band = pl.pallas_call(
        band_kernel,
        out_shape=jax.ShapeDtypeStruct((CHIPS, NARROW, 2 * YB, 128), jnp.bfloat16),
        in_specs=[smem, vmem, vmem, vmem],
        out_specs=vmem,
        scratch_shapes=[pltpu.VMEM((XB * YB, 2 * N), jnp.bfloat16)],
        name="band",
    )(deapodization, deapodization, image, z_table)
    groups = [[(chip * 2 + core) * NARROW + n for chip in range(CHIPS) for n in range(NARROW)]
              for core in range(2)]
    mine = lax.all_to_all(band.reshape(CHIPS * NARROW, 2 * YB, 128), ("wide", "narrow"), 0, 0,
                          axis_index_groups=groups, tiled=True)
    other = lax.ppermute(mine, "wide", [(i, i ^ 1) for i in range(2 * CHIPS)])
    result = pl.pallas_call(
        sample_kernel,
        out_shape=jax.ShapeDtypeStruct((SLABS, 2, SAMP), jnp.float32),
        in_specs=[smem, vmem, vmem, vmem, vmem, vmem, hbm, hbm],
        out_specs=vmem,
        scratch_shapes=[
            pltpu.VMEM((ZB, N, 2 * N), jnp.bfloat16),
            pltpu.VMEM((4, G * ZB, 128), jnp.float32),
            pltpu.VMEM((SLABS, SAMP, N), jnp.bfloat16),
            pltpu.VMEM((SLABS, SAMP, N), jnp.bfloat16),
            pltpu.SemaphoreType.DMA((SLABS,)),
            pltpu.SemaphoreType.DMA((SLABS,)),
        ],
        compiler_params=pltpu.CompilerParams(vmem_limit_bytes=60 * 1024 * 1024),
        name="samples",
    )(offsets, mine.reshape(CHIPS, NARROW * 2 * YB, 128), other.reshape(CHIPS, NARROW * 2 * YB, 128),
      y_table, x_table, phase, cross_weight[0], x_weight[0])
    return result[None]


def solution(mesh):
    return jax.shard_map(
        per_device,
        mesh=mesh,
        in_specs=(
            P(None, "wide", "narrow", None),
            P(),
            P(("wide", "narrow"), None),
            P(("wide", "narrow"), None, None, None),
            P(("wide", "narrow"), None, None, None),
        ),
        out_specs=P(("wide", "narrow"), None, None, None),
        check_vma=False,
    )
```

```python
import math

import jax
import jax.numpy as jnp
import numpy as np
from jax import lax
from jax.experimental import pallas as pl
from jax.experimental.pallas import tpu as pltpu
from jax.sharding import PartitionSpec as P

N = 256
G = 512
KZ = 64
SAMP = 1536
SLABS = 16
NARROW = 8
CHIPS = 8
XB = 16
YB = 32
ZB = KZ // NARROW


def trig(frequency, position):
    phase = np.mod(np.asarray(frequency, np.int64)[:, None] * np.asarray(position, np.int64)[None, :], G)
    angle = phase.astype(np.float32) * np.float32(2.0 * math.pi / G)
    factor = np.float32(1.0 / math.sqrt(N))
    return (np.cos(angle) * factor).astype(np.float32), (np.sin(angle) * factor).astype(np.float32)


def complex_table(cosine, sine):
    real = np.stack([cosine, sine], axis=1)
    imag = np.stack([-sine, cosine], axis=1)
    return np.stack([real, imag], axis=0)


def tables():
    position = np.arange(N) - N // 2
    z = complex_table(*trig(np.arange(KZ) - KZ // 2, position))
    z = z.reshape(2, NARROW, ZB, 2, N).transpose(3, 4, 2, 1, 0).reshape(2 * N, ZB * NARROW * 2)
    y = complex_table(*trig(np.arange(G) - G // 2, position))
    y = y.reshape(2, G, 2, NARROW, YB).transpose(0, 1, 3, 2, 4).reshape(2 * G, 2 * N)
    order = np.arange(N).reshape(CHIPS, 2, XB).transpose(1, 0, 2).reshape(N)
    x = complex_table(*trig(np.arange(N) - G // 2, position[order]))
    x = x.reshape(2 * N, 2, 2, N // 2)
    x = np.stack([x, x[:, :, ::-1]]).reshape(2, 2 * N, 2 * N)
    pc, ps = trig(np.arange(N + 8), position[order])
    phase = np.concatenate([pc, ps], axis=1) * np.float32(math.sqrt(N))
    as_bf16 = lambda t: jnp.asarray(t, jnp.float32).astype(jnp.bfloat16)
    return as_bf16(z), as_bf16(y), as_bf16(x), jnp.asarray(phase, jnp.float32)


def nt(a, b):
    return lax.dot_general(a, b, (((1,), (1,)), ((), ())), preferred_element_type=jnp.float32)


def load_all(pairs, sems):
    loads = [pltpu.make_async_copy(source, target, sems.at[i]) for i, (source, target) in enumerate(pairs)]
    for load in loads:
        load.start()
    for load in loads:
        load.wait()


def band_kernel(scale_hbm, image_hbm, z_hbm, out, scale_s, scale_v, image, z_table, rows, sems):
    wide = lax.axis_index("wide")
    narrow = lax.axis_index("narrow")
    load_all([(scale_hbm, scale_s), (scale_hbm, scale_v), (image_hbm, image), (z_hbm, z_table)], sems)
    lane = lax.broadcasted_iota(jnp.int32, (YB, N), 1)
    row = lax.broadcasted_iota(jnp.int32, (YB, N), 0)
    picked = jnp.where(lane == row + narrow * YB, scale_v[1:2, :], 0.0)
    scale_y = jnp.sum(picked, axis=1, keepdims=True)
    scale_z = scale_v[2:3, :]
    for x in range(XB):
        scale_x = scale_s[0, wide * XB + x]
        for c in range(2):
            value = image[c, x].astype(jnp.float32) * scale_x * scale_y * scale_z
            rows[x * YB:(x + 1) * YB, c * N:(c + 1) * N] = value.astype(jnp.bfloat16)
    product = jnp.dot(rows[...], z_table[...], preferred_element_type=jnp.float32)
    part = [product[x * YB:(x + 1) * YB] for x in range(XB)]
    lanes = lax.broadcasted_iota(jnp.int32, (YB, 128), 1)
    for bit in range(4):
        d = 1 << bit
        low = (lanes & d) == 0
        for i in range(XB):
            if i & d:
                continue
            a, b = part[i], part[i | d]
            part[i] = jnp.where(low, a, pltpu.roll(b, d, 1))
            part[i | d] = jnp.where(low, pltpu.roll(a, 128 - d, 1), b)
    for g in range(2 * NARROW):
        value = part[g].astype(jnp.bfloat16)
        for chip in range(CHIPS):
            out[chip, g // 2, (g % 2) * YB:(g % 2 + 1) * YB, :] = value


def table_kernel(offsets_hbm, phase_hbm, y_hbm, x_hbm, y_table, x_table, turn, offsets, phase, sems):
    core = lax.rem(lax.axis_index("wide"), 2)
    load_all([(offsets_hbm, offsets), (phase_hbm, phase), (y_hbm, y_table), (x_hbm.at[core], x_table)], sems)
    for s in range(SLABS):
        found = phase[pl.ds(offsets[0, s], 1), :]
        swapped = jnp.concatenate([found[:, 128:256], found[:, 0:128], found[:, 384:512], found[:, 256:384]], axis=1)
        turn[s:s + 1, :] = jnp.where(core == 0, found, swapped)


def transform_lines(source, y_table, turned, out):
    for chip in range(CHIPS):
        flat = source[chip].T
        for k in range(ZB):
            turned[k, chip * XB:(chip + 1) * XB, :] = flat[k * XB:(k + 1) * XB]
    for k in range(0, ZB, 2):
        lines = nt(y_table[...], turned[k:k + 2].reshape(N, 2 * N))
        for part in range(2):
            for i in range(2):
                out[part, pl.ds(k + i, G, stride=ZB), :] = lines[part * G:(part + 1) * G, i * 128:(i + 1) * 128]


def line_kernel(source, y_table, out, turned):
    transform_lines(source, y_table, turned, out)


def sample_kernel(own, other, y_table, x_table, turn, cross_hbm, gain_hbm, out,
                  rest, turned, cross, gain, even, odd, cross_sem, gain_sem):
    for s in range(SLABS):
        pltpu.make_async_copy(cross_hbm.at[s], cross.at[s], cross_sem.at[s]).start()
        pltpu.make_async_copy(gain_hbm.at[s], gain.at[s], gain_sem.at[s]).start()
    transform_lines(other, y_table, turned, rest)

    def window(s, ref):
        angle = turn[pl.ds(s, 1), :]
        start = pl.multiple_of(s * N, N)
        real_parts, imag_parts = [], []
        for half, columns in enumerate((own, rest)):
            cosine = angle[:, half * 128:(half + 1) * 128]
            sine = angle[:, N + half * 128:N + (half + 1) * 128]
            real = columns[0, pl.ds(start, N), :]
            imag = columns[1, pl.ds(start, N), :]
            real_parts.append((real * cosine + imag * sine).astype(jnp.bfloat16))
            imag_parts.append((imag * cosine - real * sine).astype(jnp.bfloat16))
        value = jnp.concatenate(real_parts + imag_parts, axis=1)
        ref[...] = nt(x_table[...], value).astype(jnp.bfloat16)

    def gather_rows(s, ref):
        for t in range(SAMP // N):
            cut = slice(t * N, (t + 1) * N)
            partial = nt(ref[...], cross[s, cut, :])
            weight = gain[s, cut, :].T.astype(jnp.float32)
            out[s, 0:1, cut] = jnp.sum(partial[:N] * weight, axis=0, keepdims=True)
            out[s, 1:2, cut] = jnp.sum(partial[N:] * weight, axis=0, keepdims=True)

    def arrive(s):
        pltpu.make_async_copy(cross_hbm.at[s], cross.at[s], cross_sem.at[s]).wait()
        pltpu.make_async_copy(gain_hbm.at[s], gain.at[s], gain_sem.at[s]).wait()

    window(0, even)

    def two_slabs(i, carry):
        s = 2 * i
        arrive(s)
        arrive(s + 1)
        gather_rows(s, even)
        window(s + 1, odd)
        gather_rows(s + 1, odd)
        window(jnp.minimum(s + 2, SLABS - 1), even)
        return carry

    lax.fori_loop(0, SLABS // 2, two_slabs, 0)


def per_device(image, deapodization, offsets, cross_weight, x_weight):
    z_table, y_table, x_table, phase = tables()
    vmem = pl.BlockSpec(memory_space=pltpu.VMEM)
    hbm = pl.BlockSpec(memory_space=pltpu.HBM)
    mib = 1024 * 1024
    band = pl.pallas_call(
        band_kernel,
        out_shape=jax.ShapeDtypeStruct((CHIPS, NARROW, 2 * YB, 128), jnp.bfloat16),
        in_specs=[hbm] * 3,
        out_specs=vmem,
        scratch_shapes=[
            pltpu.SMEM((3, N), jnp.float32),
            pltpu.VMEM((3, N), jnp.float32),
            pltpu.VMEM((2, XB, YB, N), jnp.bfloat16),
            pltpu.VMEM((2 * N, 128), jnp.bfloat16),
            pltpu.VMEM((XB * YB, 2 * N), jnp.bfloat16),
            pltpu.SemaphoreType.DMA((4,)),
        ],
        compiler_params=pltpu.CompilerParams(vmem_limit_bytes=61 * mib),
        name="band",
    )(deapodization, image, z_table)
    y_table, x_table, turn = pl.pallas_call(
        table_kernel,
        out_shape=[
            jax.ShapeDtypeStruct((2 * G, 2 * N), jnp.bfloat16),
            jax.ShapeDtypeStruct((2 * N, 2 * N), jnp.bfloat16),
            jax.ShapeDtypeStruct((SLABS, 2 * N), jnp.float32),
        ],
        in_specs=[hbm] * 4,
        out_specs=[vmem] * 3,
        scratch_shapes=[
            pltpu.SMEM((1, SLABS), jnp.int32),
            pltpu.VMEM((N + 8, 2 * N), jnp.float32),
            pltpu.SemaphoreType.DMA((4,)),
        ],
        compiler_params=pltpu.CompilerParams(vmem_limit_bytes=8 * mib),
        name="tables",
    )(offsets, phase, y_table, x_table)
    groups = [[(chip * 2 + core) * NARROW + n for chip in range(CHIPS) for n in range(NARROW)]
              for core in range(2)]
    mine = lax.all_to_all(band.reshape(CHIPS * NARROW, 2 * YB, 128), ("wide", "narrow"), 0, 0,
                          axis_index_groups=groups, tiled=True)
    mine, y_table, x_table, turn = lax.optimization_barrier((mine, y_table, x_table, turn))
    other = lax.ppermute(mine, "wide", [(i, i ^ 1) for i in range(2 * CHIPS)])
    blocks = (CHIPS, NARROW * 2 * YB, 128)
    own = pl.pallas_call(
        line_kernel,
        out_shape=jax.ShapeDtypeStruct((2, G * ZB, 128), jnp.float32),
        in_specs=[vmem, vmem],
        out_specs=vmem,
        scratch_shapes=[pltpu.VMEM((ZB, 128, 2 * N), jnp.bfloat16)],
        compiler_params=pltpu.CompilerParams(vmem_limit_bytes=16 * mib),
        cost_estimate=pl.CostEstimate(flops=2 ** 30, bytes_accessed=6 * mib, transcendentals=0),
        name="lines",
    )(mine.reshape(blocks), y_table)
    result = pl.pallas_call(
        sample_kernel,
        out_shape=jax.ShapeDtypeStruct((SLABS, 2, SAMP), jnp.float32),
        in_specs=[vmem] * 5 + [hbm] * 2,
        out_specs=vmem,
        scratch_shapes=[
            pltpu.VMEM((2, G * ZB, 128), jnp.float32),
            pltpu.VMEM((ZB, 128, 2 * N), jnp.bfloat16),
            pltpu.VMEM((SLABS, SAMP, N), jnp.bfloat16),
            pltpu.VMEM((SLABS, SAMP, N), jnp.bfloat16),
            pltpu.VMEM((2 * N, N), jnp.bfloat16),
            pltpu.VMEM((2 * N, N), jnp.bfloat16),
            pltpu.SemaphoreType.DMA((SLABS,)),
            pltpu.SemaphoreType.DMA((SLABS,)),
        ],
        compiler_params=pltpu.CompilerParams(vmem_limit_bytes=44 * mib),
        name="samples",
    )(own, other.reshape(blocks), y_table, x_table, turn, cross_weight[0], x_weight[0])
    return result[None]


def solution(mesh):
    return jax.shard_map(
        per_device,
        mesh=mesh,
        in_specs=(
            P(None, "wide", "narrow", None),
            P(),
            P(("wide", "narrow"), None),
            P(("wide", "narrow"), None, None, None),
            P(("wide", "narrow"), None, None, None),
        ),
        out_specs=P(("wide", "narrow"), None, None, None),
        check_vma=False,
    )
```

```python
import math

import jax
import jax.numpy as jnp
import numpy as np
from jax import lax
from jax.experimental import pallas as pl
from jax.experimental.pallas import tpu as pltpu
from jax.sharding import PartitionSpec as P

N = 256
G = 512
KZ = 64
SAMP = 1536
SLABS = 16
STEP = 4
NARROW = 8
CHIPS = 8
XB = 16
YB = 32
ZB = KZ // NARROW


def trig(frequency, position):
    phase = np.mod(np.asarray(frequency, np.int64)[:, None] * np.asarray(position, np.int64)[None, :], G)
    angle = phase.astype(np.float32) * np.float32(2.0 * math.pi / G)
    factor = np.float32(1.0 / math.sqrt(N))
    return (np.cos(angle) * factor).astype(np.float32), (np.sin(angle) * factor).astype(np.float32)


def complex_table(cosine, sine):
    real = np.stack([cosine, sine], axis=1)
    imag = np.stack([-sine, cosine], axis=1)
    return np.stack([real, imag], axis=0)


def tables():
    position = np.arange(N) - N // 2
    z = complex_table(*trig(np.arange(KZ) - KZ // 2, position))
    z = z.reshape(2, NARROW, ZB, 2, N).transpose(3, 4, 2, 1, 0).reshape(2 * N, ZB * NARROW * 2)
    y = complex_table(*trig(np.arange(G) - G // 2, position))
    y = y.reshape(2, G, 2, NARROW, YB).transpose(0, 1, 3, 2, 4).reshape(2 * G, 2 * N)
    order = np.arange(N).reshape(CHIPS, 2, XB).transpose(1, 0, 2).reshape(N)
    x = complex_table(*trig(np.arange(N) - G // 2, position[order]))
    x = x.reshape(2 * N, 2 * N)
    pc, ps = trig(np.arange(N + 8), position[order])
    phase = np.concatenate([pc, ps], axis=1) * np.float32(math.sqrt(N))
    as_bf16 = lambda t: jnp.asarray(t, jnp.float32).astype(jnp.bfloat16)
    return as_bf16(z), as_bf16(y), as_bf16(x), jnp.asarray(phase, jnp.float32)


def exchange_order():
    spots = [(x, y, z) for x in range(4) for y in range(4) for z in range(4)][::-1]
    spots = spots[16:] + spots[:16]
    return [(x // 2 * 4 + y, z * 2 + x % 2) for x, y, z in spots]


SPOTS = exchange_order()
WHERE = {spot: i for i, spot in enumerate(SPOTS)}


def in_hbm(*arrays):
    return [pltpu.with_memory_space_constraint(array, pltpu.HBM) for array in arrays]


def nt(a, b):
    return lax.dot_general(a, b, (((1,), (1,)), ((), ())), preferred_element_type=jnp.float32)


def load_all(pairs, sems):
    loads = [pltpu.make_async_copy(source, target, sems.at[i]) for i, (source, target) in enumerate(pairs)]
    for load in loads:
        load.start()
    for load in loads:
        load.wait()


def band_kernel(scale_hbm, image_hbm, z_hbm, out, scale_s, scale_v, image, z_table, rows, sems):
    wide = lax.axis_index("wide")
    narrow = lax.axis_index("narrow")
    load_all([(scale_hbm, scale_s), (scale_hbm, scale_v), (image_hbm, image), (z_hbm, z_table)], sems)
    lane = lax.broadcasted_iota(jnp.int32, (YB, N), 1)
    row = lax.broadcasted_iota(jnp.int32, (YB, N), 0)
    picked = jnp.where(lane == row + narrow * YB, scale_v[1:2, :], 0.0)
    scale_y = jnp.sum(picked, axis=1, keepdims=True)
    scale_z = scale_v[2:3, :]
    for x in range(XB):
        scale_x = scale_s[0, wide * XB + x]
        for c in range(2):
            value = image[c, x].astype(jnp.float32) * scale_x * scale_y * scale_z
            rows[x * YB:(x + 1) * YB, c * N:(c + 1) * N] = value.astype(jnp.bfloat16)
    product = jnp.dot(rows[...], z_table[...], preferred_element_type=jnp.float32)
    part = [product[x * YB:(x + 1) * YB] for x in range(XB)]
    lanes = lax.broadcasted_iota(jnp.int32, (YB, 128), 1)
    for bit in range(4):
        d = 1 << bit
        low = (lanes & d) == 0
        for i in range(XB):
            if i & d:
                continue
            a, b = part[i], part[i | d]
            part[i] = jnp.where(low, a, pltpu.roll(b, d, 1))
            part[i | d] = jnp.where(low, pltpu.roll(a, 128 - d, 1), b)
    for g in range(2 * NARROW):
        value = part[g].astype(jnp.bfloat16)
        for chip in range(CHIPS):
            out[WHERE[chip, g // 2], (g % 2) * YB:(g % 2 + 1) * YB, :] = value


def table_kernel(offsets_hbm, phase_hbm, y_hbm, x_hbm, y_table, x_table, turn, offsets, phase, x_any, sems):
    core = lax.rem(lax.axis_index("wide"), 2)
    load_all([(offsets_hbm, offsets), (phase_hbm, phase), (y_hbm, y_table), (x_hbm, x_any)], sems)

    def ordered(found):
        swapped = jnp.concatenate([found[:, 128:256], found[:, 0:128], found[:, 384:512], found[:, 256:384]], axis=1)
        return jnp.where(core == 0, found, swapped)

    x_table[...] = ordered(x_any[...])
    for s in range(SLABS):
        found = phase[pl.ds(offsets[0, s], 1), :]
        turn[s:s + 1, :] = ordered(found)


def transform_lines(source, y_table, turned, out):
    for chip in range(CHIPS):
        flat = jnp.concatenate([source[WHERE[chip, n]] for n in range(NARROW)], axis=0).T
        for k in range(ZB):
            turned[k, chip * XB:(chip + 1) * XB, :] = flat[k * XB:(k + 1) * XB]
    for k in range(0, ZB, 2):
        lines = nt(y_table[...], turned[k:k + 2].reshape(N, 2 * N))
        for part in range(2):
            for i in range(2):
                out[part, pl.ds(k + i, G, stride=ZB), :] = lines[part * G:(part + 1) * G, i * 128:(i + 1) * 128]


def line_kernel(source, y_table, out, turned):
    transform_lines(source, y_table, turned, out)


def sample_kernel(own, other, y_table, x_table, turn, cross_hbm, gain_hbm, out,
                  rest, turned, cross, gain, even, odd, cross_sem, gain_sem):
    def fetch(first, last):
        for s in range(first, last):
            pltpu.make_async_copy(cross_hbm.at[s], cross.at[s], cross_sem.at[s]).start()
            pltpu.make_async_copy(gain_hbm.at[s], gain.at[s], gain_sem.at[s]).start()

    fetch(0, 4)
    transform_lines(other, y_table, turned, rest)
    fetch(4, 16)

    def window(s, ref):
        angle = turn[pl.ds(s, 1), :]
        start = pl.multiple_of(s * N, N)
        real_parts, imag_parts = [], []
        for half, columns in enumerate((own, rest)):
            cosine = angle[:, half * 128:(half + 1) * 128]
            sine = angle[:, N + half * 128:N + (half + 1) * 128]
            real = columns[0, pl.ds(start, N), :]
            imag = columns[1, pl.ds(start, N), :]
            real_parts.append((real * cosine + imag * sine).astype(jnp.bfloat16))
            imag_parts.append((imag * cosine - real * sine).astype(jnp.bfloat16))
        value = jnp.concatenate(real_parts + imag_parts, axis=1)
        ref[...] = nt(x_table[...], value).astype(jnp.bfloat16)

    def gather_rows(s, ref):
        for t in range(SAMP // N):
            cut = slice(t * N, (t + 1) * N)
            partial = nt(ref[...], cross[s, cut, :])
            weight = gain[s, cut, :].T.astype(jnp.float32)
            out[s, 0:1, cut] = jnp.sum(partial[:N] * weight, axis=0, keepdims=True)
            out[s, 1:2, cut] = jnp.sum(partial[N:] * weight, axis=0, keepdims=True)

    def some_slabs(first, count):
        for j in range(count):
            s = first + j
            pltpu.make_async_copy(cross_hbm.at[s], cross.at[s], cross_sem.at[s]).wait()
            pltpu.make_async_copy(gain_hbm.at[s], gain.at[s], gain_sem.at[s]).wait()
        for j in range(0, count, 2):
            s = first + j
            gather_rows(s, even)
            window(s + 1, odd)
            gather_rows(s + 1, odd)
            window(jnp.minimum(s + 2, SLABS - 1), even)

    window(0, even)
    some_slabs(0, 2)
    some_slabs(2, 2)

    def slabs(i, carry):
        some_slabs(STEP * (i + 1), STEP)
        return carry

    lax.fori_loop(0, SLABS // STEP - 1, slabs, 0)


def per_device(image, deapodization, offsets, cross_weight, x_weight):
    z_table, y_table, x_table, phase = tables()
    vmem = pl.BlockSpec(memory_space=pltpu.VMEM)
    hbm = pl.BlockSpec(memory_space=pltpu.HBM)
    mib = 1024 * 1024
    band = pl.pallas_call(
        band_kernel,
        out_shape=jax.ShapeDtypeStruct((len(SPOTS), 2 * YB, 128), jnp.bfloat16),
        in_specs=[hbm] * 3,
        out_specs=vmem,
        scratch_shapes=[
            pltpu.SMEM((3, N), jnp.float32),
            pltpu.VMEM((3, N), jnp.float32),
            pltpu.VMEM((2, XB, YB, N), jnp.bfloat16),
            pltpu.VMEM((2 * N, 128), jnp.bfloat16),
            pltpu.VMEM((XB * YB, 2 * N), jnp.bfloat16),
            pltpu.SemaphoreType.DMA((4,)),
        ],
        compiler_params=pltpu.CompilerParams(vmem_limit_bytes=61 * mib),
        name="band",
    )(*in_hbm(deapodization, image, z_table))
    y_table, x_table, turn = pl.pallas_call(
        table_kernel,
        out_shape=[
            jax.ShapeDtypeStruct((2 * G, 2 * N), jnp.bfloat16),
            jax.ShapeDtypeStruct((2 * N, 2 * N), jnp.bfloat16),
            jax.ShapeDtypeStruct((SLABS, 2 * N), jnp.float32),
        ],
        in_specs=[hbm] * 4,
        out_specs=[vmem] * 3,
        scratch_shapes=[
            pltpu.SMEM((1, SLABS), jnp.int32),
            pltpu.VMEM((N + 8, 2 * N), jnp.float32),
            pltpu.VMEM((2 * N, 2 * N), jnp.bfloat16),
            pltpu.SemaphoreType.DMA((4,)),
        ],
        compiler_params=pltpu.CompilerParams(vmem_limit_bytes=8 * mib),
        name="tables",
    )(*in_hbm(offsets, phase, y_table, x_table))
    groups = [[(chip * 2 + core) * NARROW + n for chip, n in SPOTS] for core in range(2)]
    mine = lax.all_to_all(band, ("wide", "narrow"), 0, 0, axis_index_groups=groups, tiled=True)
    mine, y_table, x_table, turn = lax.optimization_barrier((mine, y_table, x_table, turn))
    other = lax.ppermute(mine, "wide", [(i, i ^ 1) for i in range(2 * CHIPS)])
    own = pl.pallas_call(
        line_kernel,
        out_shape=jax.ShapeDtypeStruct((2, G * ZB, 128), jnp.float32),
        in_specs=[vmem, vmem],
        out_specs=vmem,
        scratch_shapes=[pltpu.VMEM((ZB, 128, 2 * N), jnp.bfloat16)],
        compiler_params=pltpu.CompilerParams(vmem_limit_bytes=16 * mib),
        cost_estimate=pl.CostEstimate(flops=2 ** 30, bytes_accessed=6 * mib, transcendentals=0),
        name="lines",
    )(mine, y_table)
    result = pl.pallas_call(
        sample_kernel,
        out_shape=jax.ShapeDtypeStruct((SLABS, 2, SAMP), jnp.float32),
        in_specs=[vmem] * 5 + [hbm] * 2,
        out_specs=vmem,
        scratch_shapes=[
            pltpu.VMEM((2, G * ZB, 128), jnp.float32),
            pltpu.VMEM((ZB, 128, 2 * N), jnp.bfloat16),
            pltpu.VMEM((SLABS, SAMP, N), jnp.bfloat16),
            pltpu.VMEM((SLABS, SAMP, N), jnp.bfloat16),
            pltpu.VMEM((2 * N, N), jnp.bfloat16),
            pltpu.VMEM((2 * N, N), jnp.bfloat16),
            pltpu.SemaphoreType.DMA((SLABS,)),
            pltpu.SemaphoreType.DMA((SLABS,)),
        ],
        compiler_params=pltpu.CompilerParams(vmem_limit_bytes=44 * mib),
        name="samples",
    )(own, other, y_table, x_table, turn, *in_hbm(cross_weight[0], x_weight[0]))
    return result[None]


def solution(mesh):
    return jax.shard_map(
        per_device,
        mesh=mesh,
        in_specs=(
            P(None, "wide", "narrow", None),
            P(),
            P(("wide", "narrow"), None),
            P(("wide", "narrow"), None, None, None),
            P(("wide", "narrow"), None, None, None),
        ),
        out_specs=P(("wide", "narrow"), None, None, None),
        check_vma=False,
    )
```

```python
import math

import jax
import jax.numpy as jnp
import numpy as np
from jax import lax
from jax.experimental import pallas as pl
from jax.experimental.pallas import tpu as pltpu
from jax.sharding import PartitionSpec as P

N = 256
G = 512
KZ = 64
SAMP = 1536
SLABS = 16
STEP = 4
NARROW = 8
CHIPS = 8
XB = 16
YB = 32
ZB = KZ // NARROW


def trig(frequency, position):
    phase = np.mod(np.asarray(frequency, np.int64)[:, None] * np.asarray(position, np.int64)[None, :], G)
    angle = phase.astype(np.float32) * np.float32(2.0 * math.pi / G)
    factor = np.float32(1.0 / math.sqrt(N))
    return (np.cos(angle) * factor).astype(np.float32), (np.sin(angle) * factor).astype(np.float32)


def complex_table(cosine, sine):
    real = np.stack([cosine, sine], axis=1)
    imag = np.stack([-sine, cosine], axis=1)
    return np.stack([real, imag], axis=0)


def tables():
    position = np.arange(N) - N // 2
    z = complex_table(*trig(np.arange(KZ) - KZ // 2, position))
    z = z.reshape(2, NARROW, ZB, 2, N).transpose(3, 4, 2, 1, 0).reshape(2 * N, ZB * NARROW * 2)
    y = complex_table(*trig(np.arange(G) - G // 2, position))
    y = y.reshape(2, G, 2, NARROW, YB).transpose(0, 1, 3, 2, 4).reshape(2 * G, 2 * N)
    order = np.arange(N).reshape(CHIPS, 2, XB).transpose(1, 0, 2).reshape(N)
    x = complex_table(*trig(np.arange(N) - G // 2, position[order]))
    x = x.reshape(2 * N, 2 * N)
    pc, ps = trig(np.arange(N + 8), position[order])
    phase = np.concatenate([pc, ps], axis=1) * np.float32(math.sqrt(N))
    as_bf16 = lambda t: jnp.asarray(t, jnp.float32).astype(jnp.bfloat16)
    return as_bf16(z), as_bf16(y), as_bf16(x), jnp.asarray(phase, jnp.float32)


SPOTS = [(chip, n) for chip in range(CHIPS)[::-1] for n in range(NARROW)[::-1]]
WHERE = {spot: i for i, spot in enumerate(SPOTS)}


def in_hbm(*arrays):
    return [pltpu.with_memory_space_constraint(array, pltpu.HBM) for array in arrays]


def nt(a, b):
    return lax.dot_general(a, b, (((1,), (1,)), ((), ())), preferred_element_type=jnp.float32)


def load_all(pairs, sems):
    loads = [pltpu.make_async_copy(source, target, sems.at[i]) for i, (source, target) in enumerate(pairs)]
    for load in loads:
        load.start()
    for load in loads:
        load.wait()


def band_kernel(scale_hbm, image_hbm, z_hbm, out, scale_s, scale_v, image, z_table, rows, sems):
    wide = lax.axis_index("wide")
    narrow = lax.axis_index("narrow")
    load_all([(scale_hbm, scale_s), (scale_hbm, scale_v), (image_hbm, image), (z_hbm, z_table)], sems)
    lane = lax.broadcasted_iota(jnp.int32, (YB, N), 1)
    row = lax.broadcasted_iota(jnp.int32, (YB, N), 0)
    picked = jnp.where(lane == row + narrow * YB, scale_v[1:2, :], 0.0)
    scale_y = jnp.sum(picked, axis=1, keepdims=True)
    scale_z = scale_v[2:3, :]
    for x in range(XB):
        scale_x = scale_s[0, wide * XB + x]
        for c in range(2):
            value = image[c, x].astype(jnp.float32) * scale_x * scale_y * scale_z
            rows[x * YB:(x + 1) * YB, c * N:(c + 1) * N] = value.astype(jnp.bfloat16)
    product = jnp.dot(rows[...], z_table[...], preferred_element_type=jnp.float32)
    part = [product[x * YB:(x + 1) * YB] for x in range(XB)]
    lanes = lax.broadcasted_iota(jnp.int32, (YB, 128), 1)
    for bit in range(4):
        d = 1 << bit
        low = (lanes & d) == 0
        for i in range(XB):
            if i & d:
                continue
            a, b = part[i], part[i | d]
            part[i] = jnp.where(low, a, pltpu.roll(b, d, 1))
            part[i | d] = jnp.where(low, pltpu.roll(a, 128 - d, 1), b)
    for g in range(2 * NARROW):
        value = part[g].astype(jnp.bfloat16)
        out[NARROW - 1 - g // 2, (g % 2) * YB:(g % 2 + 1) * YB, :] = value


def table_kernel(offsets_hbm, phase_hbm, y_hbm, x_hbm, y_table, x_table, turn, offsets, phase, x_any, sems):
    core = lax.rem(lax.axis_index("wide"), 2)
    load_all([(offsets_hbm, offsets), (phase_hbm, phase), (y_hbm, y_table), (x_hbm, x_any)], sems)

    def ordered(found):
        swapped = jnp.concatenate([found[:, 128:256], found[:, 0:128], found[:, 384:512], found[:, 256:384]], axis=1)
        return jnp.where(core == 0, found, swapped)

    x_table[...] = ordered(x_any[...])
    for s in range(SLABS):
        found = phase[pl.ds(offsets[0, s], 1), :]
        turn[s:s + 1, :] = ordered(found)


def transform_lines(source, y_table, turned, out):
    for chip in range(CHIPS):
        flat = jnp.concatenate([source[WHERE[chip, n]] for n in range(NARROW)], axis=0).T
        for k in range(ZB):
            turned[k, chip * XB:(chip + 1) * XB, :] = flat[k * XB:(k + 1) * XB]
    for k in range(0, ZB, 2):
        lines = nt(y_table[...], turned[k:k + 2].reshape(N, 2 * N))
        for part in range(2):
            for i in range(2):
                out[part, pl.ds(k + i, G, stride=ZB), :] = lines[part * G:(part + 1) * G, i * 128:(i + 1) * 128]


def line_kernel(source, y_table, out, turned):
    transform_lines(source, y_table, turned, out)


def sample_kernel(own, other, y_table, x_table, turn, cross_hbm, gain_hbm, out,
                  rest, turned, cross, gain, even, odd, cross_sem, gain_sem):
    def fetch(first, last):
        for s in range(first, last):
            pltpu.make_async_copy(cross_hbm.at[s], cross.at[s], cross_sem.at[s]).start()
            pltpu.make_async_copy(gain_hbm.at[s], gain.at[s], gain_sem.at[s]).start()

    fetch(0, 4)
    transform_lines(other, y_table, turned, rest)
    fetch(4, 16)

    def window(s, ref):
        angle = turn[pl.ds(s, 1), :]
        start = pl.multiple_of(s * N, N)
        real_parts, imag_parts = [], []
        for half, columns in enumerate((own, rest)):
            cosine = angle[:, half * 128:(half + 1) * 128]
            sine = angle[:, N + half * 128:N + (half + 1) * 128]
            real = columns[0, pl.ds(start, N), :]
            imag = columns[1, pl.ds(start, N), :]
            real_parts.append((real * cosine + imag * sine).astype(jnp.bfloat16))
            imag_parts.append((imag * cosine - real * sine).astype(jnp.bfloat16))
        value = jnp.concatenate(real_parts + imag_parts, axis=1)
        ref[...] = nt(x_table[...], value).astype(jnp.bfloat16)

    def gather_rows(s, ref):
        for t in range(SAMP // N):
            cut = slice(t * N, (t + 1) * N)
            partial = nt(ref[...], cross[s, cut, :])
            weight = gain[s, cut, :].T.astype(jnp.float32)
            out[s, 0:1, cut] = jnp.sum(partial[:N] * weight, axis=0, keepdims=True)
            out[s, 1:2, cut] = jnp.sum(partial[N:] * weight, axis=0, keepdims=True)

    def some_slabs(first, count):
        for j in range(count):
            s = first + j
            pltpu.make_async_copy(cross_hbm.at[s], cross.at[s], cross_sem.at[s]).wait()
            pltpu.make_async_copy(gain_hbm.at[s], gain.at[s], gain_sem.at[s]).wait()
        for j in range(0, count, 2):
            s = first + j
            gather_rows(s, even)
            window(s + 1, odd)
            gather_rows(s + 1, odd)
            window(jnp.minimum(s + 2, SLABS - 1), even)

    window(0, even)
    some_slabs(0, 2)
    some_slabs(2, 2)

    def slabs(i, carry):
        some_slabs(STEP * (i + 1), STEP)
        return carry

    lax.fori_loop(0, SLABS // STEP - 1, slabs, 0)


def per_device(image, deapodization, offsets, cross_weight, x_weight):
    z_table, y_table, x_table, phase = tables()
    vmem = pl.BlockSpec(memory_space=pltpu.VMEM)
    hbm = pl.BlockSpec(memory_space=pltpu.HBM)
    mib = 1024 * 1024
    band = pl.pallas_call(
        band_kernel,
        out_shape=jax.ShapeDtypeStruct((NARROW, 2 * YB, 128), jnp.bfloat16),
        in_specs=[hbm] * 3,
        out_specs=vmem,
        scratch_shapes=[
            pltpu.SMEM((3, N), jnp.float32),
            pltpu.VMEM((3, N), jnp.float32),
            pltpu.VMEM((2, XB, YB, N), jnp.bfloat16),
            pltpu.VMEM((2 * N, 128), jnp.bfloat16),
            pltpu.VMEM((XB * YB, 2 * N), jnp.bfloat16),
            pltpu.SemaphoreType.DMA((4,)),
        ],
        compiler_params=pltpu.CompilerParams(vmem_limit_bytes=16 * mib),
        name="band",
    )(*in_hbm(deapodization, image, z_table))
    y_table, x_table, turn = pl.pallas_call(
        table_kernel,
        out_shape=[
            jax.ShapeDtypeStruct((2 * G, 2 * N), jnp.bfloat16),
            jax.ShapeDtypeStruct((2 * N, 2 * N), jnp.bfloat16),
            jax.ShapeDtypeStruct((SLABS, 2 * N), jnp.float32),
        ],
        in_specs=[hbm] * 4,
        out_specs=[vmem] * 3,
        scratch_shapes=[
            pltpu.SMEM((1, SLABS), jnp.int32),
            pltpu.VMEM((N + 8, 2 * N), jnp.float32),
            pltpu.VMEM((2 * N, 2 * N), jnp.bfloat16),
            pltpu.SemaphoreType.DMA((4,)),
        ],
        compiler_params=pltpu.CompilerParams(vmem_limit_bytes=8 * mib),
        name="tables",
    )(*in_hbm(offsets, phase, y_table, x_table))
    groups = [[(chip * 2 + core) * NARROW + n for chip, n in SPOTS] for core in range(2)]
    band = jnp.broadcast_to(band[None], (CHIPS,) + band.shape).reshape(len(SPOTS), 2 * YB, 128)
    mine = lax.all_to_all(band, ("wide", "narrow"), 0, 0, axis_index_groups=groups, tiled=True)
    mine, y_table, x_table, turn = lax.optimization_barrier((mine, y_table, x_table, turn))
    other = lax.ppermute(mine, "wide", [(i, i ^ 1) for i in range(2 * CHIPS)])
    own = pl.pallas_call(
        line_kernel,
        out_shape=jax.ShapeDtypeStruct((2, G * ZB, 128), jnp.float32),
        in_specs=[vmem, vmem],
        out_specs=vmem,
        scratch_shapes=[pltpu.VMEM((ZB, 128, 2 * N), jnp.bfloat16)],
        compiler_params=pltpu.CompilerParams(vmem_limit_bytes=16 * mib),
        cost_estimate=pl.CostEstimate(flops=2 ** 30, bytes_accessed=6 * mib, transcendentals=0),
        name="lines",
    )(mine, y_table)
    result = pl.pallas_call(
        sample_kernel,
        out_shape=jax.ShapeDtypeStruct((SLABS, 2, SAMP), jnp.float32),
        in_specs=[vmem] * 5 + [hbm] * 2,
        out_specs=vmem,
        scratch_shapes=[
            pltpu.VMEM((2, G * ZB, 128), jnp.float32),
            pltpu.VMEM((ZB, 128, 2 * N), jnp.bfloat16),
            pltpu.VMEM((SLABS, SAMP, N), jnp.bfloat16),
            pltpu.VMEM((SLABS, SAMP, N), jnp.bfloat16),
            pltpu.VMEM((2 * N, N), jnp.bfloat16),
            pltpu.VMEM((2 * N, N), jnp.bfloat16),
            pltpu.SemaphoreType.DMA((SLABS,)),
            pltpu.SemaphoreType.DMA((SLABS,)),
        ],
        compiler_params=pltpu.CompilerParams(vmem_limit_bytes=44 * mib),
        name="samples",
    )(own, other, y_table, x_table, turn, *in_hbm(cross_weight[0], x_weight[0]))
    return result[None]


def solution(mesh):
    return jax.shard_map(
        per_device,
        mesh=mesh,
        in_specs=(
            P(None, "wide", "narrow", None),
            P(),
            P(("wide", "narrow"), None),
            P(("wide", "narrow"), None, None, None),
            P(("wide", "narrow"), None, None, None),
        ),
        out_specs=P(("wide", "narrow"), None, None, None),
        check_vma=False,
    )
```

```python
import math

import jax
import jax.numpy as jnp
import numpy as np
from jax import lax
from jax.experimental import pallas as pl
from jax.experimental.pallas import tpu as pltpu
from jax.sharding import PartitionSpec as P

N = 256
G = 512
KZ = 64
SAMP = 1536
SLABS = 16
STEP = 4
NARROW = 8
CHIPS = 8
XB = 16
YB = 32
ZB = KZ // NARROW


def trig(frequency, position):
    phase = np.mod(np.asarray(frequency, np.int64)[:, None] * np.asarray(position, np.int64)[None, :], G)
    angle = phase.astype(np.float32) * np.float32(2.0 * math.pi / G)
    factor = np.float32(1.0 / math.sqrt(N))
    return (np.cos(angle) * factor).astype(np.float32), (np.sin(angle) * factor).astype(np.float32)


def complex_table(cosine, sine):
    real = np.stack([cosine, sine], axis=1)
    imag = np.stack([-sine, cosine], axis=1)
    return np.stack([real, imag], axis=0)


def tables():
    position = np.arange(N) - N // 2
    z = complex_table(*trig(np.arange(KZ) - KZ // 2, position))
    z = z.reshape(2, NARROW, ZB, 2, N).transpose(3, 4, 2, 1, 0).reshape(2 * N, ZB * NARROW * 2)
    y = complex_table(*trig(np.arange(G) - G // 2, position))
    y = y.reshape(2, G, 2, NARROW, YB).transpose(0, 1, 3, 2, 4).reshape(2 * G, 2 * N)
    order = np.arange(N).reshape(CHIPS, 2, XB).transpose(1, 0, 2).reshape(N)
    x = complex_table(*trig(np.arange(N) - G // 2, position[order]))
    x = x.reshape(2 * N, 2 * N)
    pc, ps = trig(np.arange(N + 8), position[order])
    phase = np.concatenate([pc, ps], axis=1) * np.float32(math.sqrt(N))
    as_bf16 = lambda t: jnp.asarray(t, jnp.float32).astype(jnp.bfloat16)
    return as_bf16(z), as_bf16(y), as_bf16(x), jnp.asarray(phase, jnp.float32)


def exchange_order():
    spots = [(x, y, z) for x in range(4) for y in range(4) for z in range(4)][::-1]
    spots = spots[8:] + spots[:8]
    return [(x // 2 * 4 + y, z * 2 + x % 2) for x, y, z in spots]


SPOTS = exchange_order()
WHERE = {spot: i for i, spot in enumerate(SPOTS)}


def in_hbm(*arrays):
    return [pltpu.with_memory_space_constraint(array, pltpu.HBM) for array in arrays]


def nt(a, b):
    return lax.dot_general(a, b, (((1,), (1,)), ((), ())), preferred_element_type=jnp.float32)


def load_all(pairs, sems):
    loads = [pltpu.make_async_copy(source, target, sems.at[i]) for i, (source, target) in enumerate(pairs)]
    for load in loads:
        load.start()
    for load in loads:
        load.wait()


def band_kernel(scale_hbm, image_hbm, z_hbm, out, scale_s, scale_v, image, z_table, rows, sems):
    wide = lax.axis_index("wide")
    narrow = lax.axis_index("narrow")
    load_all([(scale_hbm, scale_s), (scale_hbm, scale_v), (image_hbm, image), (z_hbm, z_table)], sems)
    lane = lax.broadcasted_iota(jnp.int32, (YB, N), 1)
    row = lax.broadcasted_iota(jnp.int32, (YB, N), 0)
    picked = jnp.where(lane == row + narrow * YB, scale_v[1:2, :], 0.0)
    scale_y = jnp.sum(picked, axis=1, keepdims=True)
    scale_z = scale_v[2:3, :]
    for x in range(XB):
        scale_x = scale_s[0, wide * XB + x]
        for c in range(2):
            value = image[c, x].astype(jnp.float32) * scale_x * scale_y * scale_z
            rows[x * YB:(x + 1) * YB, c * N:(c + 1) * N] = value.astype(jnp.bfloat16)
    product = jnp.dot(rows[...], z_table[...], preferred_element_type=jnp.float32)
    part = [product[x * YB:(x + 1) * YB] for x in range(XB)]
    lanes = lax.broadcasted_iota(jnp.int32, (YB, 128), 1)
    for bit in range(4):
        d = 1 << bit
        low = (lanes & d) == 0
        for i in range(XB):
            if i & d:
                continue
            a, b = part[i], part[i | d]
            part[i] = jnp.where(low, a, pltpu.roll(b, d, 1))
            part[i | d] = jnp.where(low, pltpu.roll(a, 128 - d, 1), b)
    for g in range(2 * NARROW):
        value = part[g].astype(jnp.bfloat16)
        for chip in range(CHIPS):
            out[WHERE[chip, g // 2], (g % 2) * YB:(g % 2 + 1) * YB, :] = value


def table_kernel(offsets_hbm, phase_hbm, y_hbm, x_hbm, y_table, x_table, turn, offsets, phase, x_any, sems):
    core = lax.rem(lax.axis_index("wide"), 2)
    load_all([(offsets_hbm, offsets), (phase_hbm, phase), (y_hbm, y_table), (x_hbm, x_any)], sems)

    def ordered(found):
        swapped = jnp.concatenate([found[:, 128:256], found[:, 0:128], found[:, 384:512], found[:, 256:384]], axis=1)
        return jnp.where(core == 0, found, swapped)

    x_table[...] = ordered(x_any[...])
    for s in range(SLABS):
        found = phase[pl.ds(offsets[0, s], 1), :]
        turn[s:s + 1, :] = ordered(found)


def transform_lines(source, y_table, turned, out):
    for chip in range(CHIPS):
        flat = jnp.concatenate([source[WHERE[chip, n]] for n in range(NARROW)], axis=0).T
        for k in range(ZB):
            turned[k, chip * XB:(chip + 1) * XB, :] = flat[k * XB:(k + 1) * XB]
    for k in range(0, ZB, 2):
        lines = nt(y_table[...], turned[k:k + 2].reshape(N, 2 * N))
        for part in range(2):
            for i in range(2):
                out[part, pl.ds(k + i, G, stride=ZB), :] = lines[part * G:(part + 1) * G, i * 128:(i + 1) * 128]


def line_kernel(source, y_table, out, turned):
    transform_lines(source, y_table, turned, out)


def sample_kernel(own, other, y_table, x_table, turn, cross_hbm, gain_hbm, out,
                  rest, turned, cross, gain, even, odd, cross_sem, gain_sem):
    def fetch(first, last):
        for s in range(first, last):
            pltpu.make_async_copy(cross_hbm.at[s], cross.at[s], cross_sem.at[s]).start()
            pltpu.make_async_copy(gain_hbm.at[s], gain.at[s], gain_sem.at[s]).start()

    fetch(0, 4)
    transform_lines(other, y_table, turned, rest)
    fetch(4, 16)

    def window(s, ref):
        angle = turn[pl.ds(s, 1), :]
        start = pl.multiple_of(s * N, N)
        real_parts, imag_parts = [], []
        for half, columns in enumerate((own, rest)):
            cosine = angle[:, half * 128:(half + 1) * 128]
            sine = angle[:, N + half * 128:N + (half + 1) * 128]
            real = columns[0, pl.ds(start, N), :]
            imag = columns[1, pl.ds(start, N), :]
            real_parts.append((real * cosine + imag * sine).astype(jnp.bfloat16))
            imag_parts.append((imag * cosine - real * sine).astype(jnp.bfloat16))
        value = jnp.concatenate(real_parts + imag_parts, axis=1)
        ref[...] = nt(x_table[...], value).astype(jnp.bfloat16)

    def gather_rows(s, ref):
        for t in range(SAMP // N):
            cut = slice(t * N, (t + 1) * N)
            partial = nt(ref[...], cross[s, cut, :])
            weight = gain[s, cut, :].T.astype(jnp.float32)
            out[s, 0:1, cut] = jnp.sum(partial[:N] * weight, axis=0, keepdims=True)
            out[s, 1:2, cut] = jnp.sum(partial[N:] * weight, axis=0, keepdims=True)

    def some_slabs(first, count):
        for j in range(count):
            s = first + j
            pltpu.make_async_copy(cross_hbm.at[s], cross.at[s], cross_sem.at[s]).wait()
            pltpu.make_async_copy(gain_hbm.at[s], gain.at[s], gain_sem.at[s]).wait()
        for j in range(0, count, 2):
            s = first + j
            gather_rows(s, even)
            window(s + 1, odd)
            gather_rows(s + 1, odd)
            window(jnp.minimum(s + 2, SLABS - 1), even)

    window(0, even)
    some_slabs(0, 2)
    some_slabs(2, 2)

    def slabs(i, carry):
        some_slabs(STEP * (i + 1), STEP)
        return carry

    lax.fori_loop(0, SLABS // STEP - 1, slabs, 0)


def per_device(image, deapodization, offsets, cross_weight, x_weight):
    z_table, y_table, x_table, phase = tables()
    vmem = pl.BlockSpec(memory_space=pltpu.VMEM)
    hbm = pl.BlockSpec(memory_space=pltpu.HBM)
    mib = 1024 * 1024
    band = pl.pallas_call(
        band_kernel,
        out_shape=jax.ShapeDtypeStruct((len(SPOTS), 2 * YB, 128), jnp.bfloat16),
        in_specs=[hbm] * 3,
        out_specs=vmem,
        scratch_shapes=[
            pltpu.SMEM((3, N), jnp.float32),
            pltpu.VMEM((3, N), jnp.float32),
            pltpu.VMEM((2, XB, YB, N), jnp.bfloat16),
            pltpu.VMEM((2 * N, 128), jnp.bfloat16),
            pltpu.VMEM((XB * YB, 2 * N), jnp.bfloat16),
            pltpu.SemaphoreType.DMA((4,)),
        ],
        compiler_params=pltpu.CompilerParams(vmem_limit_bytes=61 * mib),
        name="band",
    )(*in_hbm(deapodization, image, z_table))
    y_table, x_table, turn = pl.pallas_call(
        table_kernel,
        out_shape=[
            jax.ShapeDtypeStruct((2 * G, 2 * N), jnp.bfloat16),
            jax.ShapeDtypeStruct((2 * N, 2 * N), jnp.bfloat16),
            jax.ShapeDtypeStruct((SLABS, 2 * N), jnp.float32),
        ],
        in_specs=[hbm] * 4,
        out_specs=[vmem] * 3,
        scratch_shapes=[
            pltpu.SMEM((1, SLABS), jnp.int32),
            pltpu.VMEM((N + 8, 2 * N), jnp.float32),
            pltpu.VMEM((2 * N, 2 * N), jnp.bfloat16),
            pltpu.SemaphoreType.DMA((4,)),
        ],
        compiler_params=pltpu.CompilerParams(vmem_limit_bytes=8 * mib),
        name="tables",
    )(*in_hbm(offsets, phase, y_table, x_table))
    groups = [[(chip * 2 + core) * NARROW + n for chip, n in SPOTS] for core in range(2)]
    mine = lax.all_to_all(band, ("wide", "narrow"), 0, 0, axis_index_groups=groups, tiled=True)
    mine, y_table, x_table, turn = lax.optimization_barrier((mine, y_table, x_table, turn))
    other = lax.ppermute(mine, "wide", [(i, i ^ 1) for i in range(2 * CHIPS)])
    own = pl.pallas_call(
        line_kernel,
        out_shape=jax.ShapeDtypeStruct((2, G * ZB, 128), jnp.float32),
        in_specs=[vmem, vmem],
        out_specs=vmem,
        scratch_shapes=[pltpu.VMEM((ZB, 128, 2 * N), jnp.bfloat16)],
        compiler_params=pltpu.CompilerParams(vmem_limit_bytes=16 * mib),
        cost_estimate=pl.CostEstimate(flops=2 ** 30, bytes_accessed=6 * mib, transcendentals=0),
        name="lines",
    )(mine, y_table)
    result = pl.pallas_call(
        sample_kernel,
        out_shape=jax.ShapeDtypeStruct((SLABS, 2, SAMP), jnp.float32),
        in_specs=[vmem] * 5 + [hbm] * 2,
        out_specs=vmem,
        scratch_shapes=[
            pltpu.VMEM((2, G * ZB, 128), jnp.float32),
            pltpu.VMEM((ZB, 128, 2 * N), jnp.bfloat16),
            pltpu.VMEM((SLABS, SAMP, N), jnp.bfloat16),
            pltpu.VMEM((SLABS, SAMP, N), jnp.bfloat16),
            pltpu.VMEM((2 * N, N), jnp.bfloat16),
            pltpu.VMEM((2 * N, N), jnp.bfloat16),
            pltpu.SemaphoreType.DMA((SLABS,)),
            pltpu.SemaphoreType.DMA((SLABS,)),
        ],
        compiler_params=pltpu.CompilerParams(vmem_limit_bytes=44 * mib),
        name="samples",
    )(own, other, y_table, x_table, turn, *in_hbm(cross_weight[0], x_weight[0]))
    return result[None]


def solution(mesh):
    return jax.shard_map(
        per_device,
        mesh=mesh,
        in_specs=(
            P(None, "wide", "narrow", None),
            P(),
            P(("wide", "narrow"), None),
            P(("wide", "narrow"), None, None, None),
            P(("wide", "narrow"), None, None, None),
        ),
        out_specs=P(("wide", "narrow"), None, None, None),
        check_vma=False,
    )
```
